1024 devices in a mesh: grp: 4 (over x_hi, core), exc: 8 (over x_lo, y), col: 32 (over z).
Axes of the slice: x: 4 (x_hi: 2, x_lo: 2; x = x_hi * 2 + x_lo), y: 4, z: 32, core: 2. Of those that a mesh axis runs over, the one named last changes fastest.
Arguments:
- window_factor: float32 [1024, 32, 512], P('exc', 'grp'), may hold values from -0.375 to 0.375
- fitted_factor: float32 [1024, 512, 512], P('exc', 'col'), may hold values from -0.5 to 0.5
- pair_amps: float32 [16, 512, 512], P(None, 'col'), may hold values from -0.1875 to 0.1875
- cycle_amps: float32 [64, 32768], P(None, ('grp', 'exc')), may hold values from -6 to 6
- panel: float32 [32768, 4096], P(('grp', 'exc'), 'col'), may hold values from -0.03125 to 0.03125
Outputs:
- sigma: float32 [64, 4096], P(('grp', 'exc'), 'col')
The draws below stay inside these ranges and needn't reach their ends.
All inputs are finite; a program needn't handle non-finite values.
Results may differ from the reference program's by a relative error of at most 0.0001.
Values sent between devices are 32-bit elements; how exact they have to be, the bound alone decides.
A program may use at most 64 MiB of HBM per device.

```python
import math
import jax
import jax.numpy as jnp
from jax import lax

V = 512
NAUX = 1024
NI = 2
NJ = 8
NA = 32
ROWS = 64
NPAIR = 16
KDIM = 32768
NCOL = 4096


def strengthened(entries, own_key, source, target, parts, factor):
    def block_of(dim):
        return (jnp.arange(entries.shape[dim]) // (entries.shape[dim] // parts)).reshape((-1,) + (1,) * (entries.ndim - 1 - dim))

    first = jax.random.permutation(own_key, parts)[block_of(target)]
    second = (block_of(target) + parts // 2) % parts
    return jnp.where((block_of(source) == first) | (block_of(source) == second), factor * entries, entries)


def block_scale(own_key, shape, cuts, smallest, high):
    loudness, own = 1.0, jax.random.fold_in(own_key, 6)
    for dim, shards_of in cuts:
        heights = jnp.exp(jax.random.uniform(jax.random.fold_in(own, dim), (shards_of,), jnp.float32, smallest / len(cuts), high / len(cuts)))
        loudness = loudness * jnp.repeat(heights, shape[dim] // shards_of).reshape([-1 if axis == dim else 1 for axis in range(len(shape))])
    return loudness


def scatter_about(stream_key, extent, deviation, most, split=(), dtype=jnp.bfloat16):
    factor_of = block_scale(stream_key, extent, split, -0.22, 0.18) if split else 1.0
    values = jax.random.normal(stream_key, extent, jnp.float32) * deviation * factor_of
    return jnp.minimum(jnp.maximum(values, -most), most).astype(dtype)


def gaussian_with(own_key, dims, scale, most, shards, heavy, held_as=jnp.bfloat16):
    array = scale * jax.random.normal(own_key, dims, jnp.float32)
    if shards:
        array = array * block_scale(own_key, dims, shards, -0.22, 0.18)
    return jnp.clip(strengthened(array, jax.random.fold_in(own_key, 3), *heavy), -most, most).astype(held_as)


def setup_inputs(seed: int = 0) -> dict:
    key_list = jax.random.split(jax.random.key(seed), 6)
    return {
        "window_factor": gaussian_with(key_list[0], (NAUX, NA, V), V ** -0.5, 0.375, ((0, 8), (1, 4)), (0, 1, 8, 2.0), jnp.float32),
        "fitted_factor": gaussian_with(key_list[1], (NAUX, V, V), V ** -0.5, 0.5, ((0, 8), (1, 32)), (1, 2, 32, 2.75), jnp.float32),
        "pair_amps": scatter_about(key_list[2], (NPAIR, V, V), NAUX ** -0.5, 0.1875, ((1, 32),), jnp.float32),
        "cycle_amps": gaussian_with(key_list[3], (ROWS, KDIM), 1.0, 6.0, ((1, 32),), (1, 0, 32, 2.75), jnp.float32),
        "panel": scatter_about(key_list[4], (KDIM, NCOL), KDIM ** -0.5, 0.03125, ((0, 32), (1, 32)), jnp.float32),
    }


def reference(window_factor, fitted_factor, pair_amps, cycle_amps, panel):
    precise = lax.Precision.HIGHEST
    block = math.gcd(NAUX, 64)
    count = NAUX // block
    amplitude = pair_amps.reshape(NI, NJ, V, V)
    windows = window_factor.reshape(count, block, NA, V)
    fitted = fitted_factor.reshape(count, block, V, V)

    def accumulate(total, pieces):
        window_part, fitted_part = pieces
        inner = jnp.einsum('pac,ijdc->aijpd', window_part, amplitude, precision=precise)
        added = jnp.einsum('aijpd,pdb->aijb', inner, fitted_part, precision=precise)
        return total + added, None

    start = jnp.zeros((NA, NI, NJ, V), jnp.float32)
    total, _ = lax.scan(accumulate, start, (windows, fitted))
    ladder = total.reshape(NA * NI, NJ * V)
    cycle = jnp.dot(cycle_amps, panel, precision=precise, preferred_element_type=jnp.float32)
    return ladder + cycle
```

```python
import jax
import jax.numpy as jnp
from jax import lax
from jax.experimental import pallas as pl
from jax.experimental.pallas import tpu as pltpu
from jax.sharding import PartitionSpec as P

MESH = pl.DeviceIdType.MESH
F32 = jnp.float32
BF16 = jnp.bfloat16
NI = 2
ORDER = (0, 1, 7, 2, 6, 3, 5, 4)


def halves(x):
    high = x.astype(BF16)
    return high, (x - high.astype(F32)).astype(BF16)


def product(a, b, contract):
    dims = (contract, ((), ()))

    def dot(u, v):
        return lax.dot_general(u, v, dims, preferred_element_type=F32)

    return dot(a[0], b[0]) + (dot(a[0], b[1]) + dot(a[1], b[0]))


def make_kernel(grps, excs, cols):
    def kernel(window, fitted, amps, cycle, panel, out, extra, wb, fb, ab, cb, pb, lh, ll, fh, fl,
               send1, recv1, csend1, crecv1, send2, recv2, csend2, crecv2,
               load, ss1, rs1, ssc1, rsc1, ss2, rs2, ssc2, rsc2, ready):
        g, e, z = lax.axis_index("grp"), lax.axis_index("exc"), lax.axis_index("col")
        aux, virts = window.shape[0], window.shape[1]
        pairs, fits = amps.shape[0], amps.shape[1]
        blocks = fitted.shape[2] // 128
        njs = pairs // NI

        loads = []
        for d in range(fits):
            loads.append(pltpu.make_async_copy(amps.at[:, d, :], ab.at[pl.ds(d * pairs, pairs), :], load.at[len(loads)]))
        for a in range(virts):
            loads.append(pltpu.make_async_copy(window.at[:, a, :], wb.at[pl.ds(a * aux, aux), :], load.at[len(loads)]))
        for d in range(fits):
            loads.append(pltpu.make_async_copy(fitted.at[:, d, :], fb.at[pl.ds(d * aux, aux), :], load.at[len(loads)]))
        loads.append(pltpu.make_async_copy(cycle, cb, load.at[len(loads)]))
        loads.append(pltpu.make_async_copy(panel, pb, load.at[len(loads)]))
        for c in loads:
            c.start()
        amp_loads, win_loads = loads[:fits], loads[fits : fits + virts]
        fit_loads, cyc_loads = loads[fits + virts : 2 * fits + virts], loads[2 * fits + virts :]

        barrier = pltpu.get_barrier_semaphore()
        near = [{"exc": e ^ k} for k in range(1, excs)] + [{"grp": g ^ k} for k in range(1, grps)]
        for peer in near:
            pl.semaphore_signal(barrier, inc=1, device_id=peer, device_id_type=MESH)

        @pl.loop(z + 1, cols)
        def _(p):
            pl.semaphore_signal(barrier, inc=1, device_id={"col": p}, device_id_type=MESH)

        for c in amp_loads:
            c.wait()
        amp = halves(ab[...])
        for a in range(0, virts, 2):
            win_loads[a].wait()
            win_loads[a + 1].wait()
            win = halves(wb[pl.ds(a * aux, 2 * aux), :])
            inner = product(amp, win, ((1,), (1,)))
            for s in range(2):
                for d in range(fits):
                    high, low = halves(inner[d * pairs : (d + 1) * pairs, s * aux : (s + 1) * aux])
                    rows, lanes = pl.ds((a + s) * pairs, pairs), pl.ds(d * aux, aux)
                    lh[rows, lanes] = high
                    ll[rows, lanes] = low

        for d in range(fits):
            fit_loads[d].wait()
            high, low = halves(fb[pl.ds(d * aux, aux), :])
            fh[pl.ds(d * aux, aux), :] = high
            fl[pl.ds(d * aux, aux), :] = low
        for n in range(0, blocks, 2):
            lanes = pl.ds(n * 128, 256)
            terms = product((lh[...], ll[...]), (fh[:, lanes], fl[:, lanes]), ((1,), (0,)))
            for q in range(excs):
                for s in range(2):
                    for i in range(NI):
                        row = q * pairs + i * njs
                        send1[pl.ds(q * njs, njs), (n + s) * NI + i, :] = terms[row : row + njs, s * 128 : (s + 1) * 128]

        pl.semaphore_wait(barrier, len(near) + z)

        first = []
        js = [lax.rem(z // blocks + (njs // 2 + t), njs) for t in ORDER]
        for p, j in enumerate(js):
            step = []
            for k in reversed(range(1, excs)):
                c = pltpu.make_async_remote_copy(send1.at[(e ^ k) * njs + j], recv1.at[k - 1, p], ss1.at[k - 1, p], rs1.at[k - 1, p],
                                                 device_id={"exc": e ^ k}, device_id_type=MESH)
                c.start()
                step.append(c)
            first.append(step)

        @pl.loop(0, z)
        def _(p):
            pl.semaphore_signal(ready, inc=1, device_id={"col": p}, device_id_type=MESH)

        for c in cyc_loads:
            c.wait()
        part = product(halves(cb[...]), halves(pb[...]), ((1,), (0,)))
        for q in range(excs):
            for h in range(grps):
                row = (h * excs + q) * NI
                csend1[q, pl.ds(h * NI, NI), :] = part[row : row + NI, :]
        step = []
        for k in reversed(range(1, excs)):
            c = pltpu.make_async_remote_copy(csend1.at[e ^ k], crecv1.at[k - 1], ssc1.at[k - 1], rsc1.at[k - 1],
                                             device_id={"exc": e ^ k}, device_id_type=MESH)
            c.start()
            step.append(c)
        first.append(step)

        def to_col(p):
            return pltpu.make_async_remote_copy(send2.at[p], recv2.at[z], ss2.at[p], rs2.at[z],
                                                device_id={"col": p}, device_id_type=MESH)

        for p, j in enumerate(js):
            for c in first[p]:
                c.wait_recv()
            total = send1[e * njs + j]
            for k in range(1, excs):
                total = total + recv1[k - 1, p]
            for n in range(blocks):
                to = j * blocks + n
                send2[to] = total[n * NI : (n + 1) * NI, :]

                @pl.when(to < z)
                def _():
                    to_col(to).start()

        for c in first[-1]:
            c.wait_recv()
        total = csend1[e]
        for k in range(1, excs):
            total = total + crecv1[k - 1]
        for h in range(grps):
            csend2[h] = total[h * NI : (h + 1) * NI, :]
        across = []
        for k in range(1, grps):
            c = pltpu.make_async_remote_copy(csend2.at[g ^ k], crecv2.at[k - 1], ssc2.at[k - 1], rsc2.at[k - 1],
                                             device_id={"grp": g ^ k}, device_id_type=MESH)
            c.start()
            across.append(c)

        @pl.when(z < cols - 1)
        def _():
            pl.semaphore_wait(ready, cols - 1 - z)

        @pl.loop(z + 1, cols)
        def _(p):
            to_col(p).start()

        for c in across:
            c.wait_recv()
        cyc = csend2[g]
        for k in range(1, grps):
            cyc = cyc + crecv2[k - 1]
        extra[...] = cyc

        def arrived(p):
            return pltpu.make_async_remote_copy(send2.at[p], recv2.at[p], ss2.at[p], rs2.at[p],
                                                device_id={"col": p}, device_id_type=MESH)

        result = send2[z]
        for k in range(1, cols):
            p = lax.rem(z + k, cols)
            arrived(p).wait_recv()
            result = result + recv2[p]
        out[...] = result
        for step in first + [across]:
            for c in step:
                c.wait_send()
        for k in range(1, cols):
            arrived(lax.rem(z + k, cols)).wait_send()

    return kernel


def solution(mesh):
    grps, excs, cols = mesh.shape["grp"], mesh.shape["exc"], mesh.shape["col"]

    def shards(window, fitted, amps, cycle, panel):
        aux, virts, virtuals = window.shape
        fits, wide = fitted.shape[1:]
        pairs = amps.shape[0]
        njs, blocks = pairs // NI, wide // 128
        DMA = pltpu.SemaphoreType.DMA
        scratch = [
            pltpu.VMEM((virts * aux, virtuals), F32),
            pltpu.VMEM((fits * aux, wide), F32),
            pltpu.VMEM((fits * pairs, virtuals), F32),
            pltpu.VMEM(cycle.shape, F32),
            pltpu.VMEM(panel.shape, F32),
            pltpu.VMEM((virts * pairs, fits * aux), BF16),
            pltpu.VMEM((virts * pairs, fits * aux), BF16),
            pltpu.VMEM((fits * aux, wide), BF16),
            pltpu.VMEM((fits * aux, wide), BF16),
            pltpu.VMEM((excs * njs, blocks * NI, 128), F32),
            pltpu.VMEM((excs - 1, njs, blocks * NI, 128), F32),
            pltpu.VMEM((excs, grps * NI, 128), F32),
            pltpu.VMEM((excs - 1, grps * NI, 128), F32),
            pltpu.VMEM((cols, NI, 128), F32),
            pltpu.VMEM((cols, NI, 128), F32),
            pltpu.VMEM((grps, NI, 128), F32),
            pltpu.VMEM((grps - 1, NI, 128), F32),
            DMA((2 * fits + virts + 2,)),
            DMA((excs - 1, njs)),
            DMA((excs - 1, njs)),
            DMA((excs - 1,)),
            DMA((excs - 1,)),
            DMA((cols,)),
            DMA((cols,)),
            DMA((grps - 1,)),
            DMA((grps - 1,)),
            pltpu.SemaphoreType.REGULAR,
        ]
        anywhere = pl.BlockSpec(memory_space=pl.ANY)
        ladder, cyc = pl.pallas_call(
            make_kernel(grps, excs, cols),
            out_shape=(jax.ShapeDtypeStruct((NI, 128), F32),) * 2,
            in_specs=[anywhere] * 5,
            out_specs=(pl.BlockSpec(memory_space=pltpu.VMEM),) * 2,
            scratch_shapes=scratch,
            compiler_params=pltpu.CompilerParams(collective_id=0, has_side_effects=True),
            name="residual",
        )(window, fitted, amps, cycle, panel)
        return ladder + cyc

    placed = (
        P("exc", "grp", None),
        P("exc", "col", None),
        P(None, "col", None),
        P(None, ("grp", "exc")),
        P(("grp", "exc"), "col"),
    )
    return jax.shard_map(
        shards, mesh=mesh, in_specs=placed, out_specs=P(("grp", "exc"), "col"), check_vma=False
    )
```

```python
import jax
import jax.numpy as jnp
from jax import lax
from jax.experimental import pallas as pl
from jax.experimental.pallas import tpu as pltpu
from jax.sharding import PartitionSpec as P

MESH = pl.DeviceIdType.MESH
F32 = jnp.float32
BF16 = jnp.bfloat16
NI = 2
GROUPS = ((0, 4), (4, 4), (8, 4), (12, 2), (14, 2))
ORDER = (0, 1, 7, 2, 6, 3, 5, 4)


def halves(x):
    high = x.astype(BF16)
    return high, (x - high.astype(F32)).astype(BF16)


def product(a, b, contract):
    dims = (contract, ((), ()))

    def dot(u, v):
        return lax.dot_general(u, v, dims, preferred_element_type=F32)

    return dot(a[0], b[0]) + (dot(a[0], b[1]) + dot(a[1], b[0]))


def make_kernel(grps, excs, cols):
    def kernel(window, fitted, amps, cycle, panel, out, extra, wb, fb, ab, cb, pb, lh, ll, acc,
               send1, recv1, csend1, crecv1, send2, recv2, csend2, crecv2,
               amp_load, win_load, fit_load, cyc_load, sent, rs1, rsc, rs2, ready):
        g, e, z = lax.axis_index("grp"), lax.axis_index("exc"), lax.axis_index("col")
        aux, virts = window.shape[0], window.shape[1]
        pairs, fits = amps.shape[0], amps.shape[1]
        blocks = fitted.shape[2] // 128
        njs = pairs // NI

        def landed(ref, sem):
            return pltpu.make_async_copy(ref, ref, sem)

        for d in range(fits):
            pltpu.make_async_copy(amps.at[:, d, :], ab.at[pl.ds(d * pairs, pairs), :], amp_load).start()
        for a in range(virts):
            pltpu.make_async_copy(window.at[:, a, :], wb.at[pl.ds(a * aux, aux), :], win_load.at[a // 2]).start()
        for t, (d0, nd) in enumerate(GROUPS):
            for d in range(d0, d0 + nd):
                pltpu.make_async_copy(fitted.at[:, d, :], fb.at[pl.ds(d * aux, aux), :], fit_load.at[t]).start()
        pltpu.make_async_copy(cycle, cb, cyc_load.at[0]).start()
        pltpu.make_async_copy(panel, pb, cyc_load.at[1]).start()

        barrier = pltpu.get_barrier_semaphore()
        near = [{"exc": e ^ k} for k in range(1, excs)] + [{"grp": g ^ k} for k in range(1, grps)]
        for peer in near:
            pl.semaphore_signal(barrier, inc=1, device_id=peer, device_id_type=MESH)

        @pl.loop(z + 1, cols)
        def _(p):
            pl.semaphore_signal(barrier, inc=1, device_id={"col": p}, device_id_type=MESH)

        landed(ab, amp_load).wait()
        amp = halves(ab[...])
        for a in range(0, virts, 2):
            both = pl.ds(a * aux, 2 * aux)
            landed(wb.at[both, :], win_load.at[a // 2]).wait()
            inner = product(amp, halves(wb[both, :]), ((1,), (1,)))
            for s in range(2):
                for d in range(fits):
                    high, low = halves(inner[d * pairs : (d + 1) * pairs, s * aux : (s + 1) * aux])
                    rows, lanes = pl.ds((a + s) * pairs, pairs), pl.ds(d * aux, aux)
                    lh[rows, lanes] = high
                    ll[rows, lanes] = low

        for t, (d0, nd) in enumerate(GROUPS):
            deep = pl.ds(d0 * aux, nd * aux)
            landed(fb.at[deep, :], fit_load.at[t]).wait()
            for n in range(0, blocks, 2):
                lanes = pl.ds(n * 128, 256)
                terms = product((lh[:, deep], ll[:, deep]), halves(fb[deep, lanes]), ((1,), (0,)))
                if t:
                    terms = terms + acc[:, lanes]
                if t < len(GROUPS) - 1:
                    acc[:, lanes] = terms
                    continue
                for q in range(excs):
                    for s in range(2):
                        for i in range(NI):
                            row = q * pairs + i * njs
                            send1[pl.ds(q * njs, njs), (n + s) * NI + i, :] = terms[row : row + njs, s * 128 : (s + 1) * 128]

        pl.semaphore_wait(barrier, len(near) + z)

        js = [lax.rem(z // blocks + (njs // 2 + t), njs) for t in ORDER]
        for p, j in enumerate(js):
            for k in reversed(range(1, excs)):
                pltpu.make_async_remote_copy(send1.at[(e ^ k) * njs + j], recv1.at[p, k - 1], sent.at[0], rs1.at[p],
                                             device_id={"exc": e ^ k}, device_id_type=MESH).start()

        @pl.loop(0, z)
        def _(p):
            pl.semaphore_signal(ready, inc=1, device_id={"col": p}, device_id_type=MESH)

        landed(cb, cyc_load.at[0]).wait()
        landed(pb, cyc_load.at[1]).wait()
        part = product(halves(cb[...]), halves(pb[...]), ((1,), (0,)))
        for q in range(excs):
            for h in range(grps):
                row = (h * excs + q) * NI
                csend1[q, pl.ds(h * NI, NI), :] = part[row : row + NI, :]
        for k in reversed(range(1, excs)):
            pltpu.make_async_remote_copy(csend1.at[e ^ k], crecv1.at[k - 1], sent.at[1], rsc.at[0],
                                         device_id={"exc": e ^ k}, device_id_type=MESH).start()

        def to_col(p):
            return pltpu.make_async_remote_copy(send2.at[p], recv2.at[lax.rem(p - z - 1 + cols, cols)], sent.at[2], rs2,
                                                device_id={"col": p}, device_id_type=MESH)

        for p, j in enumerate(js):
            landed(recv1.at[p], rs1.at[p]).wait()
            total = send1[e * njs + j]
            for k in range(1, excs):
                total = total + recv1[p, k - 1]
            for n in range(blocks):
                to = j * blocks + n
                send2[to] = total[n * NI : (n + 1) * NI, :]

                @pl.when(to < z)
                def _():
                    to_col(to).start()

        landed(crecv1, rsc.at[0]).wait()
        total = csend1[e]
        for k in range(1, excs):
            total = total + crecv1[k - 1]
        for h in range(grps):
            csend2[h] = total[h * NI : (h + 1) * NI, :]
        for k in range(1, grps):
            pltpu.make_async_remote_copy(csend2.at[g ^ k], crecv2.at[k - 1], sent.at[3], rsc.at[1],
                                         device_id={"grp": g ^ k}, device_id_type=MESH).start()

        @pl.when(z < cols - 1)
        def _():
            pl.semaphore_wait(ready, cols - 1 - z)

        @pl.loop(z + 1, cols)
        def _(p):
            to_col(p).start()

        landed(crecv2, rsc.at[1]).wait()
        cyc = csend2[g]
        for k in range(1, grps):
            cyc = cyc + crecv2[k - 1]
        extra[...] = cyc
        for t, (ref, own) in enumerate(((send1, njs), (csend1, 1), (send2, 1), (csend2, 1))):
            landed(ref.at[pl.ds(0, ref.shape[0] - own)], sent.at[t]).wait()
        landed(recv2, rs2).wait()
        result = send2[z]
        for k in range(1, cols):
            result = result + recv2[k - 1]
        out[...] = result

    return kernel


def solution(mesh):
    grps, excs, cols = mesh.shape["grp"], mesh.shape["exc"], mesh.shape["col"]

    def shards(window, fitted, amps, cycle, panel):
        aux, virts, virtuals = window.shape
        fits, wide = fitted.shape[1:]
        pairs = amps.shape[0]
        njs, blocks = pairs // NI, wide // 128
        DMA = pltpu.SemaphoreType.DMA
        scratch = [
            pltpu.VMEM((virts * aux, virtuals), F32),
            pltpu.VMEM((fits * aux, wide), F32),
            pltpu.VMEM((fits * pairs, virtuals), F32),
            pltpu.VMEM(cycle.shape, F32),
            pltpu.VMEM(panel.shape, F32),
            pltpu.VMEM((virts * pairs, fits * aux), BF16),
            pltpu.VMEM((virts * pairs, fits * aux), BF16),
            pltpu.VMEM((virts * pairs, wide), F32),
            pltpu.VMEM((excs * njs, blocks * NI, 128), F32),
            pltpu.VMEM((njs, excs - 1, blocks * NI, 128), F32),
            pltpu.VMEM((excs, grps * NI, 128), F32),
            pltpu.VMEM((excs - 1, grps * NI, 128), F32),
            pltpu.VMEM((cols, NI, 128), F32),
            pltpu.VMEM((cols - 1, NI, 128), F32),
            pltpu.VMEM((grps, NI, 128), F32),
            pltpu.VMEM((grps - 1, NI, 128), F32),
            DMA,
            DMA((virts // 2,)),
            DMA((len(GROUPS),)),
            DMA((2,)),
            DMA((4,)),
            DMA((njs,)),
            DMA((2,)),
            DMA,
            pltpu.SemaphoreType.REGULAR,
        ]
        anywhere = pl.BlockSpec(memory_space=pl.ANY)
        ladder, cyc = pl.pallas_call(
            make_kernel(grps, excs, cols),
            out_shape=(pltpu.VMEM((NI, 128), F32),) * 2,
            in_specs=[anywhere] * 5,
            out_specs=(pl.BlockSpec(memory_space=pltpu.VMEM),) * 2,
            scratch_shapes=scratch,
            compiler_params=pltpu.CompilerParams(collective_id=0, has_side_effects=True),
            name="residual",
        )(window, fitted, amps, cycle, panel)
        return ladder + cyc

    placed = (
        P("exc", "grp", None),
        P("exc", "col", None),
        P(None, "col", None),
        P(None, ("grp", "exc")),
        P(("grp", "exc"), "col"),
    )
    return jax.shard_map(
        shards, mesh=mesh, in_specs=placed, out_specs=P(("grp", "exc"), "col"), check_vma=False
    )
```

```python
import jax
import jax.numpy as jnp
from jax import lax
from jax.experimental import pallas as pl
from jax.experimental.pallas import tpu as pltpu
from jax.sharding import PartitionSpec as P

MESH = pl.DeviceIdType.MESH
F32 = jnp.float32
BF16 = jnp.bfloat16
NI = 2
GROUPS = ((0, 4), (4, 4), (8, 4), (12, 2), (14, 2))
ORDER = (0, 1, 7, 2, 6, 3, 5, 4)


def halves(x):
    high = x.astype(BF16)
    return high, (x - high.astype(F32)).astype(BF16)


def product(a, b, contract):
    dims = (contract, ((), ()))

    def dot(u, v):
        return lax.dot_general(u, v, dims, preferred_element_type=F32)

    return dot(a[0], b[0]) + (dot(a[0], b[1]) + dot(a[1], b[0]))


def make_kernel(grps, excs, cols):
    def kernel(window, fitted, amps, cycle, panel, out, extra, wb, fb, ab, cb, pb, lh, ll, acc,
               send1, recv1, csend1, crecv1, send2, recv2, csend2, crecv2, direct,
               amp_load, win_load, fit_load, cyc_load, sent, rs1, rsc, rs2, rsd, ready):
        g, e, z = lax.axis_index("grp"), lax.axis_index("exc"), lax.axis_index("col")
        aux, virts = window.shape[0], window.shape[1]
        pairs, fits = amps.shape[0], amps.shape[1]
        blocks = fitted.shape[2] // 128
        njs = pairs // NI

        def landed(ref, sem):
            return pltpu.make_async_copy(ref, ref, sem)

        for d in range(fits):
            pltpu.make_async_copy(amps.at[:, d, :], ab.at[pl.ds(d * pairs, pairs), :], amp_load).start()
        for a in range(virts):
            pltpu.make_async_copy(window.at[:, a, :], wb.at[pl.ds(a * aux, aux), :], win_load.at[a // 2]).start()
        for t, (d0, nd) in enumerate(GROUPS):
            for d in range(d0, d0 + nd):
                pltpu.make_async_copy(fitted.at[:, d, :], fb.at[pl.ds(d * aux, aux), :], fit_load.at[t]).start()
        pltpu.make_async_copy(cycle, cb, cyc_load.at[0]).start()
        pltpu.make_async_copy(panel, pb, cyc_load.at[1]).start()

        half = cols // 2
        lower = z < half
        known = jnp.minimum(z, half)
        barrier = pltpu.get_barrier_semaphore()
        near = [{"exc": e ^ k} for k in range(1, excs)] + [{"grp": g ^ k} for k in range(1, grps)]
        for peer in near:
            pl.semaphore_signal(barrier, inc=1, device_id=peer, device_id_type=MESH)

        source = (z >= half) & (z < half + blocks)
        target = z < blocks

        @pl.when(target)
        def _():
            for k in range(1, excs):
                for t in range(blocks):
                    pl.semaphore_signal(barrier, inc=1, device_id={"exc": e ^ k, "col": half + t}, device_id_type=MESH)

        @pl.when(lower)
        def _():
            @pl.loop(z + 1, cols)
            def _(p):
                pl.semaphore_signal(barrier, inc=1, device_id={"col": p}, device_id_type=MESH)

        landed(ab, amp_load).wait()
        amp = halves(ab[...])
        for a in range(0, virts, 2):
            both = pl.ds(a * aux, 2 * aux)
            landed(wb.at[both, :], win_load.at[a // 2]).wait()
            inner = product(amp, halves(wb[both, :]), ((1,), (1,)))
            for s in range(2):
                for d in range(fits):
                    high, low = halves(inner[d * pairs : (d + 1) * pairs, s * aux : (s + 1) * aux])
                    rows, lanes = pl.ds((a + s) * pairs, pairs), pl.ds(d * aux, aux)
                    lh[rows, lanes] = high
                    ll[rows, lanes] = low

        for t, (d0, nd) in enumerate(GROUPS):
            deep = pl.ds(d0 * aux, nd * aux)
            landed(fb.at[deep, :], fit_load.at[t]).wait()
            for n in range(0, blocks, 2):
                lanes = pl.ds(n * 128, 256)
                terms = product((lh[:, deep], ll[:, deep]), halves(fb[deep, lanes]), ((1,), (0,)))
                if t:
                    terms = terms + acc[:, lanes]
                if t < len(GROUPS) - 1:
                    acc[:, lanes] = terms
                    continue
                for q in range(excs):
                    for s in range(2):
                        for i in range(NI):
                            row = q * pairs + i * njs
                            send1[pl.ds(q * njs, njs), (n + s) * NI + i, :] = terms[row : row + njs, s * 128 : (s + 1) * 128]

        pl.semaphore_wait(barrier, len(near) + known + jnp.where(source, (excs - 1) * blocks, 0))

        @pl.when(source)
        def _():
            for t in range(blocks):
                for k in reversed(range(excs)):
                    pltpu.make_async_remote_copy(send1.at[(e ^ k) * njs, pl.ds(t * NI, NI), :], direct.at[(z - half) * excs + e],
                                                 sent.at[4], rsd, device_id={"exc": e ^ k, "col": t}, device_id_type=MESH).start()

        def to_exc(p, j):
            for k in reversed(range(1, excs)):
                pltpu.make_async_remote_copy(send1.at[(e ^ k) * njs + j], recv1.at[p, k - 1], sent.at[0], rs1.at[p],
                                             device_id={"exc": e ^ k}, device_id_type=MESH).start()

        js = [lax.rem(z // blocks + (njs // 2 + t), njs) for t in ORDER]

        @pl.when(jnp.logical_not(source))
        def _():
            to_exc(0, js[0])

        for p in range(1, njs):
            to_exc(p, js[p])

        @pl.loop(0, known)
        def _(p):
            pl.semaphore_signal(ready, inc=1, device_id={"col": p}, device_id_type=MESH)

        landed(cb, cyc_load.at[0]).wait()
        landed(pb, cyc_load.at[1]).wait()
        part = product(halves(cb[...]), halves(pb[...]), ((1,), (0,)))
        for q in range(excs):
            for h in range(grps):
                row = (h * excs + q) * NI
                csend1[q, pl.ds(h * NI, NI), :] = part[row : row + NI, :]
        for k in reversed(range(1, excs)):
            pltpu.make_async_remote_copy(csend1.at[e ^ k], crecv1.at[k - 1], sent.at[1], rsc.at[0],
                                         device_id={"exc": e ^ k}, device_id_type=MESH).start()

        def to_col(p):
            return pltpu.make_async_remote_copy(send2.at[p], recv2.at[lax.rem(p - z - 1 + cols, cols)], sent.at[2], rs2,
                                                device_id={"col": p}, device_id_type=MESH)

        def reduce_to_cols(p, j):
            landed(recv1.at[p], rs1.at[p]).wait()
            total = send1[e * njs + j]
            for k in range(1, excs):
                total = total + recv1[p, k - 1]
            for n in range(blocks):
                to = j * blocks + n
                send2[to] = total[n * NI : (n + 1) * NI, :]

                @pl.when(to < known)
                def _():
                    to_col(to).start()

        @pl.when(jnp.logical_not(source))
        def _():
            reduce_to_cols(0, js[0])

        for p in range(1, njs):
            reduce_to_cols(p, js[p])

        landed(crecv1, rsc.at[0]).wait()
        total = csend1[e]
        for k in range(1, excs):
            total = total + crecv1[k - 1]
        for h in range(grps):
            csend2[h] = total[h * NI : (h + 1) * NI, :]
        for k in range(1, grps):
            pltpu.make_async_remote_copy(csend2.at[g ^ k], crecv2.at[k - 1], sent.at[3], rsc.at[1],
                                         device_id={"grp": g ^ k}, device_id_type=MESH).start()

        pl.semaphore_wait(ready, jnp.where(lower, cols - 1 - z, 1))
        for teller, start in ((half - 1, half), (0, half + half // 2)):

            @pl.when(z == teller)
            def _():
                @pl.loop(start, start + half // 2)
                def _(p):
                    pl.semaphore_signal(ready, inc=1, device_id={"col": p}, device_id_type=MESH)

        @pl.loop(jnp.where(lower, z + 1, half), cols)
        def _(p):
            @pl.when(p != z)
            def _():
                to_col(p).start()

        landed(crecv2, rsc.at[1]).wait()
        cyc = csend2[g]
        for k in range(1, grps):
            cyc = cyc + crecv2[k - 1]
        extra[...] = cyc
        def all_sent(t, ref, count):
            landed(ref.at[pl.ds(0, count)], sent.at[t]).wait()

        @pl.when(source)
        def _():
            all_sent(0, send1, (excs - 1) * (njs - 1))
            all_sent(2, send2, cols - 1 - blocks)
            all_sent(4, direct, excs * blocks)

        @pl.when(jnp.logical_not(source))
        def _():
            all_sent(0, send1, (excs - 1) * njs)
            all_sent(2, send2, cols - 1)

        all_sent(1, csend1, excs - 1)
        all_sent(3, csend2, grps - 1)

        @pl.when(target)
        def _():
            landed(recv2.at[pl.ds(0, cols - 1 - blocks)], rs2).wait()
            landed(direct, rsd).wait()
            for t in range(blocks):
                plane = direct[t * excs]
                for k in range(1, excs):
                    plane = plane + direct[t * excs + k]
                recv2[lax.rem(z - (half + t) - 1 + cols, cols)] = plane

        @pl.when(jnp.logical_not(target))
        def _():
            landed(recv2, rs2).wait()

        result = send2[z]
        for k in range(1, cols):
            result = result + recv2[k - 1]
        out[...] = result

    return kernel


def solution(mesh):
    grps, excs, cols = mesh.shape["grp"], mesh.shape["exc"], mesh.shape["col"]

    def shards(window, fitted, amps, cycle, panel):
        aux, virts, virtuals = window.shape
        fits, wide = fitted.shape[1:]
        pairs = amps.shape[0]
        njs, blocks = pairs // NI, wide // 128
        DMA = pltpu.SemaphoreType.DMA
        scratch = [
            pltpu.VMEM((virts * aux, virtuals), F32),
            pltpu.VMEM((fits * aux, wide), F32),
            pltpu.VMEM((fits * pairs, virtuals), F32),
            pltpu.VMEM(cycle.shape, F32),
            pltpu.VMEM(panel.shape, F32),
            pltpu.VMEM((virts * pairs, fits * aux), BF16),
            pltpu.VMEM((virts * pairs, fits * aux), BF16),
            pltpu.VMEM((virts * pairs, wide), F32),
            pltpu.VMEM((excs * njs, blocks * NI, 128), F32),
            pltpu.VMEM((njs, excs - 1, blocks * NI, 128), F32),
            pltpu.VMEM((excs, grps * NI, 128), F32),
            pltpu.VMEM((excs - 1, grps * NI, 128), F32),
            pltpu.VMEM((cols, NI, 128), F32),
            pltpu.VMEM((cols - 1, NI, 128), F32),
            pltpu.VMEM((grps, NI, 128), F32),
            pltpu.VMEM((grps - 1, NI, 128), F32),
            pltpu.VMEM((excs * blocks, NI, 128), F32),
            DMA,
            DMA((virts // 2,)),
            DMA((len(GROUPS),)),
            DMA((2,)),
            DMA((5,)),
            DMA((njs,)),
            DMA((2,)),
            DMA,
            DMA,
            pltpu.SemaphoreType.REGULAR,
        ]
        anywhere = pl.BlockSpec(memory_space=pl.ANY)
        ladder, cyc = pl.pallas_call(
            make_kernel(grps, excs, cols),
            out_shape=(pltpu.VMEM((NI, 128), F32),) * 2,
            in_specs=[anywhere] * 5,
            out_specs=(pl.BlockSpec(memory_space=pltpu.VMEM),) * 2,
            scratch_shapes=scratch,
            compiler_params=pltpu.CompilerParams(collective_id=0, has_side_effects=True),
            name="residual",
        )(window, fitted, amps, cycle, panel)
        return ladder + cyc

    placed = (
        P("exc", "grp", None),
        P("exc", "col", None),
        P(None, "col", None),
        P(None, ("grp", "exc")),
        P(("grp", "exc"), "col"),
    )
    return jax.shard_map(
        shards, mesh=mesh, in_specs=placed, out_specs=P(("grp", "exc"), "col"), check_vma=False
    )
```

```python
import jax
import jax.numpy as jnp
from jax import lax
from jax.experimental import pallas as pl
from jax.experimental.pallas import tpu as pltpu
from jax.sharding import PartitionSpec as P

MESH = pl.DeviceIdType.MESH
F32 = jnp.float32
BF16 = jnp.bfloat16
NI = 2
GROUPS = ((0, 10), (10, 6))
ORDER = (0, 1, 7, 2, 6, 3, 5, 4)


def halves(x):
    high = x.astype(BF16)
    return high, (x - high.astype(F32)).astype(BF16)


def product(a, b, contract):
    dims = (contract, ((), ()))

    def dot(u, v):
        return lax.dot_general(u, v, dims, preferred_element_type=F32)

    return dot(a[0], b[0]) + (dot(a[0], b[1]) + dot(a[1], b[0]))


def make_kernel(grps, excs, cols):
    def kernel(window, fitted, amps, cycle, panel, out, extra, wb, fb, ab, cb, pb, lh, ll, acc,
               send1, recv1, csend1, crecv1, send2, recv2, csend2, crecv2, direct,
               amp_load, win_load, fit_load, cyc_load, sent, rs1, rsc, rs2, rsd, ready):
        g, e, z = lax.axis_index("grp"), lax.axis_index("exc"), lax.axis_index("col")
        aux, virts = window.shape[0], window.shape[1]
        pairs, fits = amps.shape[0], amps.shape[1]
        blocks = fitted.shape[2] // 128
        njs = pairs // NI

        def landed(ref, sem):
            return pltpu.make_async_copy(ref, ref, sem)

        for d in range(fits):
            pltpu.make_async_copy(amps.at[:, d, :], ab.at[pl.ds(d * pairs, pairs), :], amp_load).start()
        for a in range(virts):
            pltpu.make_async_copy(window.at[:, a, :], wb.at[pl.ds(a * aux, aux), :], win_load).start()
        for t, (d0, nd) in enumerate(GROUPS):
            for d in range(d0, d0 + nd):
                pltpu.make_async_copy(fitted.at[:, d, :], fb.at[pl.ds(d * aux, aux), :], fit_load.at[t]).start()
        pltpu.make_async_copy(cycle, cb, cyc_load.at[0]).start()
        pltpu.make_async_copy(panel, pb, cyc_load.at[1]).start()

        half = cols // 2
        lower = z < half
        known = jnp.minimum(z, half)
        barrier = pltpu.get_barrier_semaphore()
        near = [{"exc": e ^ k} for k in range(1, excs)] + [{"grp": g ^ k} for k in range(1, grps)]
        for peer in near:
            pl.semaphore_signal(barrier, inc=1, device_id=peer, device_id_type=MESH)

        source = (z >= half) & (z < half + blocks)
        target = z < blocks

        @pl.when(target)
        def _():
            for k in range(1, excs):
                for t in range(blocks):
                    pl.semaphore_signal(barrier, inc=1, device_id={"exc": e ^ k, "col": half + t}, device_id_type=MESH)

        @pl.when(lower)
        def _():
            @pl.loop(z + 1, cols)
            def _(p):
                pl.semaphore_signal(barrier, inc=1, device_id={"col": p}, device_id_type=MESH)

        landed(ab, amp_load).wait()
        landed(wb, win_load).wait()
        amp = halves(ab[...])
        for a in range(0, virts, 2):
            both = pl.ds(a * aux, 2 * aux)
            inner = product(amp, halves(wb[both, :]), ((1,), (1,)))
            for s in range(2):
                for d in range(fits):
                    high, low = halves(inner[d * pairs : (d + 1) * pairs, s * aux : (s + 1) * aux])
                    rows, lanes = pl.ds((a + s) * pairs, pairs), pl.ds(d * aux, aux)
                    lh[rows, lanes] = high
                    ll[rows, lanes] = low

        pl.semaphore_wait(barrier, len(near) + known + jnp.where(source, (excs - 1) * blocks, 0))

        @pl.loop(0, known)
        def _(p):
            pl.semaphore_signal(ready, inc=1, device_id={"col": p}, device_id_type=MESH)

        for t, (d0, nd) in enumerate(GROUPS):
            deep = pl.ds(d0 * aux, nd * aux)
            landed(fb.at[deep, :], fit_load.at[t]).wait()
            for n in range(0, blocks, 2):
                lanes = pl.ds(n * 128, 256)
                terms = product((lh[:, deep], ll[:, deep]), halves(fb[deep, lanes]), ((1,), (0,)))
                if t:
                    terms = terms + acc[:, lanes]
                if t < len(GROUPS) - 1:
                    acc[:, lanes] = terms
                    continue
                for q in range(excs):
                    for s in range(2):
                        for i in range(NI):
                            row = q * pairs + i * njs
                            send1[pl.ds(q * njs, njs), (n + s) * NI + i, :] = terms[row : row + njs, s * 128 : (s + 1) * 128]

        @pl.when(source)
        def _():
            for t in range(blocks):
                for k in reversed(range(excs)):
                    pltpu.make_async_remote_copy(send1.at[(e ^ k) * njs, pl.ds(t * NI, NI), :], direct.at[(z - half) * excs + e],
                                                 sent.at[4], rsd, device_id={"exc": e ^ k, "col": t}, device_id_type=MESH).start()

        def to_exc(p, j):
            for k in reversed(range(1, excs)):
                pltpu.make_async_remote_copy(send1.at[(e ^ k) * njs + j], recv1.at[p, k - 1], sent.at[0], rs1.at[p],
                                             device_id={"exc": e ^ k}, device_id_type=MESH).start()

        js = [lax.rem(z // blocks + (njs // 2 + t), njs) for t in ORDER]

        @pl.when(jnp.logical_not(source))
        def _():
            to_exc(0, js[0])

        for p in range(1, njs):
            to_exc(p, js[p])

        landed(cb, cyc_load.at[0]).wait()
        landed(pb, cyc_load.at[1]).wait()
        part = product(halves(cb[...]), halves(pb[...]), ((1,), (0,)))
        for q in range(excs):
            for h in range(grps):
                row = (h * excs + q) * NI
                csend1[q, pl.ds(h * NI, NI), :] = part[row : row + NI, :]
        for k in reversed(range(1, excs)):
            pltpu.make_async_remote_copy(csend1.at[e ^ k], crecv1.at[k - 1], sent.at[1], rsc.at[0],
                                         device_id={"exc": e ^ k}, device_id_type=MESH).start()

        def to_col(p):
            return pltpu.make_async_remote_copy(send2.at[p], recv2.at[lax.rem(p - z - 1 + cols, cols)], sent.at[2], rs2,
                                                device_id={"col": p}, device_id_type=MESH)

        def reduce_to_cols(p, j):
            landed(recv1.at[p], rs1.at[p]).wait()
            total = send1[e * njs + j]
            for k in range(1, excs):
                total = total + recv1[p, k - 1]
            for n in range(blocks):
                to = j * blocks + n
                send2[to] = total[n * NI : (n + 1) * NI, :]

                @pl.when(to < known)
                def _():
                    to_col(to).start()

        @pl.when(jnp.logical_not(source))
        def _():
            reduce_to_cols(0, js[0])

        for p in range(1, njs):
            reduce_to_cols(p, js[p])

        landed(crecv1, rsc.at[0]).wait()
        total = csend1[e]
        for k in range(1, excs):
            total = total + crecv1[k - 1]
        for h in range(grps):
            csend2[h] = total[h * NI : (h + 1) * NI, :]
        for k in range(1, grps):
            pltpu.make_async_remote_copy(csend2.at[g ^ k], crecv2.at[k - 1], sent.at[3], rsc.at[1],
                                         device_id={"grp": g ^ k}, device_id_type=MESH).start()

        pl.semaphore_wait(ready, jnp.where(lower, cols - 1 - z, 1))
        for teller, start in ((half - 1, half), (0, half + half // 2)):

            @pl.when(z == teller)
            def _():
                @pl.loop(start, start + half // 2)
                def _(p):
                    pl.semaphore_signal(ready, inc=1, device_id={"col": p}, device_id_type=MESH)

        @pl.loop(jnp.where(lower, z + 1, half), cols)
        def _(p):
            @pl.when(p != z)
            def _():
                to_col(p).start()

        landed(crecv2, rsc.at[1]).wait()
        cyc = csend2[g]
        for k in range(1, grps):
            cyc = cyc + crecv2[k - 1]
        extra[...] = cyc
        def all_sent(t, ref, count):
            landed(ref.at[pl.ds(0, count)], sent.at[t]).wait()

        @pl.when(source)
        def _():
            all_sent(0, send1, (excs - 1) * (njs - 1))
            all_sent(2, send2, cols - 1 - blocks)
            all_sent(4, direct, excs * blocks)

        @pl.when(jnp.logical_not(source))
        def _():
            all_sent(0, send1, (excs - 1) * njs)
            all_sent(2, send2, cols - 1)

        all_sent(1, csend1, excs - 1)
        all_sent(3, csend2, grps - 1)

        @pl.when(target)
        def _():
            landed(recv2.at[pl.ds(0, cols - 1 - blocks)], rs2).wait()
            landed(direct, rsd).wait()
            for t in range(blocks):
                plane = direct[t * excs]
                for k in range(1, excs):
                    plane = plane + direct[t * excs + k]
                recv2[lax.rem(z - (half + t) - 1 + cols, cols)] = plane

        @pl.when(jnp.logical_not(target))
        def _():
            landed(recv2, rs2).wait()

        result = send2[z]
        for k in range(1, cols):
            result = result + recv2[k - 1]
        out[...] = result

    return kernel


def solution(mesh):
    grps, excs, cols = mesh.shape["grp"], mesh.shape["exc"], mesh.shape["col"]

    def shards(window, fitted, amps, cycle, panel):
        aux, virts, virtuals = window.shape
        fits, wide = fitted.shape[1:]
        pairs = amps.shape[0]
        njs, blocks = pairs // NI, wide // 128
        DMA = pltpu.SemaphoreType.DMA
        scratch = [
            pltpu.VMEM((virts * aux, virtuals), F32),
            pltpu.VMEM((fits * aux, wide), F32),
            pltpu.VMEM((fits * pairs, virtuals), F32),
            pltpu.VMEM(cycle.shape, F32),
            pltpu.VMEM(panel.shape, F32),
            pltpu.VMEM((virts * pairs, fits * aux), BF16),
            pltpu.VMEM((virts * pairs, fits * aux), BF16),
            pltpu.VMEM((virts * pairs, wide), F32),
            pltpu.VMEM((excs * njs, blocks * NI, 128), F32),
            pltpu.VMEM((njs, excs - 1, blocks * NI, 128), F32),
            pltpu.VMEM((excs, grps * NI, 128), F32),
            pltpu.VMEM((excs - 1, grps * NI, 128), F32),
            pltpu.VMEM((cols, NI, 128), F32),
            pltpu.VMEM((cols - 1, NI, 128), F32),
            pltpu.VMEM((grps, NI, 128), F32),
            pltpu.VMEM((grps - 1, NI, 128), F32),
            pltpu.VMEM((excs * blocks, NI, 128), F32),
            DMA,
            DMA,
            DMA((len(GROUPS),)),
            DMA((2,)),
            DMA((5,)),
            DMA((njs,)),
            DMA((2,)),
            DMA,
            DMA,
            pltpu.SemaphoreType.REGULAR,
        ]
        anywhere = pl.BlockSpec(memory_space=pl.ANY)
        ladder, cyc = pl.pallas_call(
            make_kernel(grps, excs, cols),
            out_shape=(pltpu.VMEM((NI, 128), F32),) * 2,
            in_specs=[anywhere] * 5,
            out_specs=(pl.BlockSpec(memory_space=pltpu.VMEM),) * 2,
            scratch_shapes=scratch,
            compiler_params=pltpu.CompilerParams(collective_id=0, has_side_effects=True),
            name="residual",
        )(window, fitted, amps, cycle, panel)
        return ladder + cyc

    placed = (
        P("exc", "grp", None),
        P("exc", "col", None),
        P(None, "col", None),
        P(None, ("grp", "exc")),
        P(("grp", "exc"), "col"),
    )
    return jax.shard_map(
        shards, mesh=mesh, in_specs=placed, out_specs=P(("grp", "exc"), "col"), check_vma=False
    )
```

```python
import jax
import jax.numpy as jnp
from jax import lax
from jax.experimental import pallas as pl
from jax.experimental.pallas import tpu as pltpu
from jax.sharding import PartitionSpec as P

MESH = pl.DeviceIdType.MESH
F32 = jnp.float32
BF16 = jnp.bfloat16
NI = 2
GROUPS = ((0, 10), (10, 6))
ORDER = (0, 1, 7, 2, 6, 3, 5, 4)


def halves(x):
    high = x.astype(BF16)
    return high, (x - high.astype(F32)).astype(BF16)


def product(a, b, contract):
    dims = (contract, ((), ()))

    def dot(u, v):
        return lax.dot_general(u, v, dims, preferred_element_type=F32)

    return dot(a[0], b[0]) + (dot(a[0], b[1]) + dot(a[1], b[0]))


def make_kernel(grps, excs, cols):
    def kernel(window, fitted, amps, cycle, panel, out, extra, wb, fb, ab, cb, pb, lh, ll, acc,
               send1, recv1, csend1, crecv1, send2, recv2, csend2, crecv2, direct,
               amp_load, win_load, fit_load, cyc_load, sent, rs1, rsc, rs2, rsd, ready):
        g, e, z = lax.axis_index("grp"), lax.axis_index("exc"), lax.axis_index("col")
        aux, virts = window.shape[0], window.shape[1]
        pairs, fits = amps.shape[0], amps.shape[1]
        blocks = fitted.shape[2] // 128
        njs = pairs // NI

        def landed(ref, sem):
            return pltpu.make_async_copy(ref, ref, sem)

        for d in range(fits):
            pltpu.make_async_copy(amps.at[:, d, :], ab.at[pl.ds(d * pairs, pairs), :], amp_load).start()
        for a in range(virts):
            pltpu.make_async_copy(window.at[:, a, :], wb.at[pl.ds(a * aux, aux), :], win_load).start()
        for t, (d0, nd) in enumerate(GROUPS):
            for d in range(d0, d0 + nd):
                pltpu.make_async_copy(fitted.at[:, d, :], fb.at[pl.ds(d * aux, aux), :], fit_load.at[t]).start()
        pltpu.make_async_copy(cycle, cb, cyc_load.at[0]).start()
        pltpu.make_async_copy(panel, pb, cyc_load.at[1]).start()

        half = cols // 2
        lower = z < half
        known = jnp.minimum(z, half)
        barrier = pltpu.get_barrier_semaphore()
        near = [{"exc": e ^ k} for k in range(1, excs)] + [{"grp": g ^ k} for k in range(1, grps)]
        for peer in near:
            pl.semaphore_signal(barrier, inc=1, device_id=peer, device_id_type=MESH)

        source = (z >= half) & (z < half + blocks)
        target = z < blocks

        @pl.when(target)
        def _():
            for k in range(1, excs):
                for t in range(blocks):
                    pl.semaphore_signal(barrier, inc=1, device_id={"exc": e ^ k, "col": half + t}, device_id_type=MESH)

        @pl.when(lower)
        def _():
            @pl.loop(z + 1, cols)
            def _(p):
                pl.semaphore_signal(barrier, inc=1, device_id={"col": p}, device_id_type=MESH)

        landed(ab, amp_load).wait()
        landed(wb, win_load).wait()
        amp = halves(ab[...])
        for a in range(0, virts, 2):
            both = pl.ds(a * aux, 2 * aux)
            inner = product(amp, halves(wb[both, :]), ((1,), (1,)))
            for s in range(2):
                for d in range(fits):
                    high, low = halves(inner[d * pairs : (d + 1) * pairs, s * aux : (s + 1) * aux])
                    rows, lanes = pl.ds((a + s) * pairs, pairs), pl.ds(d * aux, aux)
                    lh[rows, lanes] = high
                    ll[rows, lanes] = low

        for t, (d0, nd) in enumerate(GROUPS):
            deep = pl.ds(d0 * aux, nd * aux)
            landed(fb.at[deep, :], fit_load.at[t]).wait()
            for n in range(0, blocks, 2):
                lanes = pl.ds(n * 128, 256)
                terms = product((lh[:, deep], ll[:, deep]), halves(fb[deep, lanes]), ((1,), (0,)))
                if t:
                    terms = terms + acc[:, lanes]
                if t < len(GROUPS) - 1:
                    acc[:, lanes] = terms
                    continue
                for q in range(excs):
                    for s in range(2):
                        for i in range(NI):
                            row = q * pairs + i * njs
                            send1[pl.ds(q * njs, njs), (n + s) * NI + i, :] = terms[row : row + njs, s * 128 : (s + 1) * 128]

        pl.semaphore_wait(barrier, len(near) + known + jnp.where(source, (excs - 1) * blocks, 0))

        @pl.when(source)
        def _():
            for t in range(blocks):
                for k in reversed(range(excs)):
                    pltpu.make_async_remote_copy(send1.at[(e ^ k) * njs, pl.ds(t * NI, NI), :], direct.at[(z - half) * excs + e],
                                                 sent.at[4], rsd, device_id={"exc": e ^ k, "col": t}, device_id_type=MESH).start()

        def to_exc(p, j):
            for k in reversed(range(1, excs)):
                pltpu.make_async_remote_copy(send1.at[(e ^ k) * njs + j], recv1.at[p, k - 1], sent.at[0], rs1.at[p],
                                             device_id={"exc": e ^ k}, device_id_type=MESH).start()

        js = [lax.rem(z // blocks + (njs // 2 + t), njs) for t in ORDER]

        @pl.when(jnp.logical_not(source))
        def _():
            to_exc(0, js[0])

        for p in range(1, njs):
            to_exc(p, js[p])

        @pl.loop(0, known)
        def _(p):
            pl.semaphore_signal(ready, inc=1, device_id={"col": p}, device_id_type=MESH)

        landed(cb, cyc_load.at[0]).wait()
        landed(pb, cyc_load.at[1]).wait()
        part = product(halves(cb[...]), halves(pb[...]), ((1,), (0,)))
        for q in range(excs):
            for h in range(grps):
                row = (h * excs + q) * NI
                csend1[q, pl.ds(h * NI, NI), :] = part[row : row + NI, :]
        for k in reversed(range(1, excs)):
            pltpu.make_async_remote_copy(csend1.at[e ^ k], crecv1.at[k - 1], sent.at[1], rsc.at[0],
                                         device_id={"exc": e ^ k}, device_id_type=MESH).start()

        def to_col(p):
            return pltpu.make_async_remote_copy(send2.at[p], recv2.at[lax.rem(p - z - 1 + cols, cols)], sent.at[2], rs2,
                                                device_id={"col": p}, device_id_type=MESH)

        def reduce_to_cols(p, j):
            landed(recv1.at[p], rs1.at[p]).wait()
            total = send1[e * njs + j]
            for k in range(1, excs):
                total = total + recv1[p, k - 1]
            for n in range(blocks):
                to = j * blocks + n
                send2[to] = total[n * NI : (n + 1) * NI, :]

                @pl.when(to < known)
                def _():
                    to_col(to).start()

        @pl.when(jnp.logical_not(source))
        def _():
            reduce_to_cols(0, js[0])

        for p in range(1, njs):
            reduce_to_cols(p, js[p])

        landed(crecv1, rsc.at[0]).wait()
        total = csend1[e]
        for k in range(1, excs):
            total = total + crecv1[k - 1]
        for h in range(grps):
            csend2[h] = total[h * NI : (h + 1) * NI, :]
        for k in range(1, grps):
            pltpu.make_async_remote_copy(csend2.at[g ^ k], crecv2.at[k - 1], sent.at[3], rsc.at[1],
                                         device_id={"grp": g ^ k}, device_id_type=MESH).start()

        pl.semaphore_wait(ready, jnp.where(lower, cols - 1 - z, 1))
        for teller, start in ((half - 1, half), (0, half + half // 2)):

            @pl.when(z == teller)
            def _():
                @pl.loop(start, start + half // 2)
                def _(p):
                    pl.semaphore_signal(ready, inc=1, device_id={"col": p}, device_id_type=MESH)

        @pl.loop(jnp.where(lower, z + 1, half), cols)
        def _(p):
            @pl.when(p != z)
            def _():
                to_col(p).start()

        landed(crecv2, rsc.at[1]).wait()
        cyc = csend2[g]
        for k in range(1, grps):
            cyc = cyc + crecv2[k - 1]
        extra[...] = cyc
        def all_sent(t, ref, count):
            landed(ref.at[pl.ds(0, count)], sent.at[t]).wait()

        @pl.when(source)
        def _():
            all_sent(0, send1, (excs - 1) * (njs - 1))
            all_sent(2, send2, cols - 1 - blocks)
            all_sent(4, direct, excs * blocks)

        @pl.when(jnp.logical_not(source))
        def _():
            all_sent(0, send1, (excs - 1) * njs)
            all_sent(2, send2, cols - 1)

        all_sent(1, csend1, excs - 1)
        all_sent(3, csend2, grps - 1)

        @pl.when(target)
        def _():
            landed(recv2.at[pl.ds(0, cols - 1 - blocks)], rs2).wait()
            landed(direct, rsd).wait()
            for t in range(blocks):
                plane = direct[t * excs]
                for k in range(1, excs):
                    plane = plane + direct[t * excs + k]
                recv2[lax.rem(z - (half + t) - 1 + cols, cols)] = plane

        @pl.when(jnp.logical_not(target))
        def _():
            landed(recv2, rs2).wait()

        result = send2[z]
        for k in range(1, cols):
            result = result + recv2[k - 1]
        out[...] = result

    return kernel


def solution(mesh):
    grps, excs, cols = mesh.shape["grp"], mesh.shape["exc"], mesh.shape["col"]

    def shards(window, fitted, amps, cycle, panel):
        aux, virts, virtuals = window.shape
        fits, wide = fitted.shape[1:]
        pairs = amps.shape[0]
        njs, blocks = pairs // NI, wide // 128
        DMA = pltpu.SemaphoreType.DMA
        scratch = [
            pltpu.VMEM((virts * aux, virtuals), F32),
            pltpu.VMEM((fits * aux, wide), F32),
            pltpu.VMEM((fits * pairs, virtuals), F32),
            pltpu.VMEM(cycle.shape, F32),
            pltpu.VMEM(panel.shape, F32),
            pltpu.VMEM((virts * pairs, fits * aux), BF16),
            pltpu.VMEM((virts * pairs, fits * aux), BF16),
            pltpu.VMEM((virts * pairs, wide), F32),
            pltpu.VMEM((excs * njs, blocks * NI, 128), F32),
            pltpu.VMEM((njs, excs - 1, blocks * NI, 128), F32),
            pltpu.VMEM((excs, grps * NI, 128), F32),
            pltpu.VMEM((excs - 1, grps * NI, 128), F32),
            pltpu.VMEM((cols, NI, 128), F32),
            pltpu.VMEM((cols - 1, NI, 128), F32),
            pltpu.VMEM((grps, NI, 128), F32),
            pltpu.VMEM((grps - 1, NI, 128), F32),
            pltpu.VMEM((excs * blocks, NI, 128), F32),
            DMA,
            DMA,
            DMA((len(GROUPS),)),
            DMA((2,)),
            DMA((5,)),
            DMA((njs,)),
            DMA((2,)),
            DMA,
            DMA,
            pltpu.SemaphoreType.REGULAR,
        ]
        anywhere = pl.BlockSpec(memory_space=pl.ANY)
        ladder, cyc = pl.pallas_call(
            make_kernel(grps, excs, cols),
            out_shape=(pltpu.VMEM((NI, 128), F32),) * 2,
            in_specs=[anywhere] * 5,
            out_specs=(pl.BlockSpec(memory_space=pltpu.VMEM),) * 2,
            scratch_shapes=scratch,
            compiler_params=pltpu.CompilerParams(collective_id=0, has_side_effects=True),
            name="residual",
        )(window, fitted, amps, cycle, panel)
        return ladder + cyc

    placed = (
        P("exc", "grp", None),
        P("exc", "col", None),
        P(None, "col", None),
        P(None, ("grp", "exc")),
        P(("grp", "exc"), "col"),
    )
    return jax.shard_map(
        shards, mesh=mesh, in_specs=placed, out_specs=P(("grp", "exc"), "col"), check_vma=False
    )
```

```python
import jax
import jax.numpy as jnp
from jax import lax
from jax.experimental import pallas as pl
from jax.experimental.pallas import tpu as pltpu
from jax.sharding import PartitionSpec as P

MESH = pl.DeviceIdType.MESH
F32 = jnp.float32
BF16 = jnp.bfloat16
NI = 2
GROUPS = ((0, 10), (10, 6))


def halves(x):
    high = x.astype(BF16)
    return high, (x - high.astype(F32)).astype(BF16)


def product(a, b, contract):
    dims = (contract, ((), ()))

    def dot(u, v):
        return lax.dot_general(u, v, dims, preferred_element_type=F32)

    return dot(a[0], b[0]) + (dot(a[0], b[1]) + dot(a[1], b[0]))


def make_kernel(grps, excs, cols):
    def kernel(window, fitted, amps, cycle, panel, out, extra, wb, fb, ab, cb, pb, lh, ll, acc,
               send1, recv1, csend1, crecv1, send2, recv2, csend2, crecv2, direct,
               amp_load, win_load, fit_load, cyc_load, sent, rs1, rsc, rs2, rsd, ready):
        g, e, z = lax.axis_index("grp"), lax.axis_index("exc"), lax.axis_index("col")
        aux, virts = window.shape[0], window.shape[1]
        pairs, fits = amps.shape[0], amps.shape[1]
        blocks = fitted.shape[2] // 128
        njs = pairs // NI

        def landed(ref, sem):
            return pltpu.make_async_copy(ref, ref, sem)

        for d in range(fits):
            pltpu.make_async_copy(amps.at[:, d, :], ab.at[pl.ds(d * pairs, pairs), :], amp_load).start()
        for a in range(virts):
            pltpu.make_async_copy(window.at[:, a, :], wb.at[pl.ds(a * aux, aux), :], win_load).start()
        for t, (d0, nd) in enumerate(GROUPS):
            for d in range(d0, d0 + nd):
                pltpu.make_async_copy(fitted.at[:, d, :], fb.at[pl.ds(d * aux, aux), :], fit_load.at[t]).start()
        pltpu.make_async_copy(cycle, cb, cyc_load.at[0]).start()
        pltpu.make_async_copy(panel, pb, cyc_load.at[1]).start()

        half = cols // 2
        lower = z < half
        known = jnp.minimum(z, half)
        barrier = pltpu.get_barrier_semaphore()
        near = [{"exc": e ^ k} for k in range(1, excs)] + [{"grp": g ^ k} for k in range(1, grps)]
        for peer in near:
            pl.semaphore_signal(barrier, inc=1, device_id=peer, device_id_type=MESH)

        source = (z >= half) & (z < half + blocks)
        target = z < blocks

        @pl.when(target)
        def _():
            for k in range(1, excs):
                for t in range(blocks):
                    pl.semaphore_signal(barrier, inc=1, device_id={"exc": e ^ k, "col": half + t}, device_id_type=MESH)

        @pl.when(lower)
        def _():
            @pl.loop(z + 1, cols)
            def _(p):
                pl.semaphore_signal(barrier, inc=1, device_id={"col": p}, device_id_type=MESH)

        landed(ab, amp_load).wait()
        landed(wb, win_load).wait()
        amp = halves(ab[...])
        for a in range(0, virts, 2):
            both = pl.ds(a * aux, 2 * aux)
            inner = product(amp, halves(wb[both, :]), ((1,), (1,)))
            for s in range(2):
                for d in range(fits):
                    high, low = halves(inner[d * pairs : (d + 1) * pairs, s * aux : (s + 1) * aux])
                    rows, lanes = pl.ds((a + s) * pairs, pairs), pl.ds(d * aux, aux)
                    lh[rows, lanes] = high
                    ll[rows, lanes] = low

        for t, (d0, nd) in enumerate(GROUPS):
            deep = pl.ds(d0 * aux, nd * aux)
            landed(fb.at[deep, :], fit_load.at[t]).wait()
            for n in range(0, blocks, 2):
                lanes = pl.ds(n * 128, 256)
                terms = product((lh[:, deep], ll[:, deep]), halves(fb[deep, lanes]), ((1,), (0,)))
                if t:
                    terms = terms + acc[:, lanes]
                if t < len(GROUPS) - 1:
                    acc[:, lanes] = terms
                    continue
                for q in range(excs):
                    for s in range(2):
                        for i in range(NI):
                            row = q * pairs + i * njs
                            send1[pl.ds(q * njs, njs), (n + s) * NI + i, :] = terms[row : row + njs, s * 128 : (s + 1) * 128]

        pl.semaphore_wait(barrier, len(near) + known + jnp.where(source, (excs - 1) * blocks, 0))

        @pl.when(source)
        def _():
            for t in range(blocks):
                for k in reversed(range(excs)):
                    pltpu.make_async_remote_copy(send1.at[(e ^ k) * njs, pl.ds(t * NI, NI), :], direct.at[(z - half) * excs + e],
                                                 sent.at[4], rsd, device_id={"exc": e ^ k, "col": t}, device_id_type=MESH).start()

        def to_exc(j):
            for k in reversed(range(1, excs)):
                pltpu.make_async_remote_copy(send1.at[(e ^ k) * njs + j], recv1.at[j, k - 1], sent.at[0], rs1.at[j],
                                             device_id={"exc": e ^ k}, device_id_type=MESH).start()

        @pl.when(jnp.logical_not(source))
        def _():
            to_exc(0)

        for p in range(1, njs):
            to_exc(p)

        @pl.loop(0, known)
        def _(p):
            pl.semaphore_signal(ready, inc=1, device_id={"col": p}, device_id_type=MESH)

        landed(cb, cyc_load.at[0]).wait()
        landed(pb, cyc_load.at[1]).wait()
        part = product(halves(cb[...]), halves(pb[...]), ((1,), (0,)))
        for q in range(excs):
            for h in range(grps):
                row = (h * excs + q) * NI
                csend1[q, pl.ds(h * NI, NI), :] = part[row : row + NI, :]
        for k in reversed(range(1, excs)):
            pltpu.make_async_remote_copy(csend1.at[e ^ k], crecv1.at[k - 1], sent.at[1], rsc.at[0],
                                         device_id={"exc": e ^ k}, device_id_type=MESH).start()

        def to_col(p):
            return pltpu.make_async_remote_copy(send2.at[p], recv2.at[lax.rem(p - z - 1 + cols, cols)], sent.at[2], rs2,
                                                device_id={"col": p}, device_id_type=MESH)

        def reduce_to_cols(j):
            landed(recv1.at[j], rs1.at[j]).wait()
            total = send1[e * njs + j]
            for k in range(1, excs):
                total = total + recv1[j, k - 1]
            for n in range(blocks):
                to = j * blocks + n
                send2[to] = total[n * NI : (n + 1) * NI, :]

                @pl.when(to < known)
                def _():
                    to_col(to).start()

        @pl.when(jnp.logical_not(source))
        def _():
            reduce_to_cols(0)

        for p in range(1, njs):
            reduce_to_cols(p)

        landed(crecv1, rsc.at[0]).wait()
        total = csend1[e]
        for k in range(1, excs):
            total = total + crecv1[k - 1]
        for h in range(grps):
            csend2[h] = total[h * NI : (h + 1) * NI, :]
        for k in range(1, grps):
            pltpu.make_async_remote_copy(csend2.at[g ^ k], crecv2.at[k - 1], sent.at[3], rsc.at[1],
                                         device_id={"grp": g ^ k}, device_id_type=MESH).start()

        pl.semaphore_wait(ready, jnp.where(lower, cols - 1 - z, 1))
        for teller, start in ((half - 1, half), (0, half + half // 2)):

            @pl.when(z == teller)
            def _():
                @pl.loop(start, start + half // 2)
                def _(p):
                    pl.semaphore_signal(ready, inc=1, device_id={"col": p}, device_id_type=MESH)

        @pl.loop(jnp.where(lower, z + 1, half), cols)
        def _(p):
            @pl.when(p != z)
            def _():
                to_col(p).start()

        landed(crecv2, rsc.at[1]).wait()
        cyc = csend2[g]
        for k in range(1, grps):
            cyc = cyc + crecv2[k - 1]
        extra[...] = cyc
        def all_sent(t, ref, count):
            landed(ref.at[pl.ds(0, count)], sent.at[t]).wait()

        @pl.when(source)
        def _():
            all_sent(0, send1, (excs - 1) * (njs - 1))
            all_sent(2, send2, cols - 1 - blocks)
            all_sent(4, direct, excs * blocks)

        @pl.when(jnp.logical_not(source))
        def _():
            all_sent(0, send1, (excs - 1) * njs)
            all_sent(2, send2, cols - 1)

        all_sent(1, csend1, excs - 1)
        all_sent(3, csend2, grps - 1)

        @pl.when(target)
        def _():
            landed(recv2.at[pl.ds(0, cols - 1 - blocks)], rs2).wait()
            landed(direct, rsd).wait()
            for t in range(blocks):
                plane = direct[t * excs]
                for k in range(1, excs):
                    plane = plane + direct[t * excs + k]
                recv2[lax.rem(z - (half + t) - 1 + cols, cols)] = plane

        @pl.when(jnp.logical_not(target))
        def _():
            landed(recv2, rs2).wait()

        result = send2[z]
        for k in range(1, cols):
            result = result + recv2[k - 1]
        out[...] = result

    return kernel


def solution(mesh):
    grps, excs, cols = mesh.shape["grp"], mesh.shape["exc"], mesh.shape["col"]

    def shards(window, fitted, amps, cycle, panel):
        aux, virts, virtuals = window.shape
        fits, wide = fitted.shape[1:]
        pairs = amps.shape[0]
        njs, blocks = pairs // NI, wide // 128
        DMA = pltpu.SemaphoreType.DMA
        scratch = [
            pltpu.VMEM((virts * aux, virtuals), F32),
            pltpu.VMEM((fits * aux, wide), F32),
            pltpu.VMEM((fits * pairs, virtuals), F32),
            pltpu.VMEM(cycle.shape, F32),
            pltpu.VMEM(panel.shape, F32),
            pltpu.VMEM((virts * pairs, fits * aux), BF16),
            pltpu.VMEM((virts * pairs, fits * aux), BF16),
            pltpu.VMEM((virts * pairs, wide), F32),
            pltpu.VMEM((excs * njs, blocks * NI, 128), F32),
            pltpu.VMEM((njs, excs - 1, blocks * NI, 128), F32),
            pltpu.VMEM((excs, grps * NI, 128), F32),
            pltpu.VMEM((excs - 1, grps * NI, 128), F32),
            pltpu.VMEM((cols, NI, 128), F32),
            pltpu.VMEM((cols - 1, NI, 128), F32),
            pltpu.VMEM((grps, NI, 128), F32),
            pltpu.VMEM((grps - 1, NI, 128), F32),
            pltpu.VMEM((excs * blocks, NI, 128), F32),
            DMA,
            DMA,
            DMA((len(GROUPS),)),
            DMA((2,)),
            DMA((5,)),
            DMA((njs,)),
            DMA((2,)),
            DMA,
            DMA,
            pltpu.SemaphoreType.REGULAR,
        ]
        anywhere = pl.BlockSpec(memory_space=pl.ANY)
        ladder, cyc = pl.pallas_call(
            make_kernel(grps, excs, cols),
            out_shape=(pltpu.VMEM((NI, 128), F32),) * 2,
            in_specs=[anywhere] * 5,
            out_specs=(pl.BlockSpec(memory_space=pltpu.VMEM),) * 2,
            scratch_shapes=scratch,
            compiler_params=pltpu.CompilerParams(collective_id=0, has_side_effects=True),
            name="residual",
        )(window, fitted, amps, cycle, panel)
        return ladder + cyc

    placed = (
        P("exc", "grp", None),
        P("exc", "col", None),
        P(None, "col", None),
        P(None, ("grp", "exc")),
        P(("grp", "exc"), "col"),
    )
    return jax.shard_map(
        shards, mesh=mesh, in_specs=placed, out_specs=P(("grp", "exc"), "col"), check_vma=False
    )
```
